128 devices in a mesh: row: 8 (over z, y_lo), col: 16 (over x, y_hi, core).
Axes of the slice: x: 4, y: 4 (y_hi: 2, y_lo: 2; y = y_hi * 2 + y_lo), z: 4, core: 2. Of those that a mesh axis runs over, the one named last changes fastest.
Arguments:
- slab_pair: float32 [65536, 4096], P('row', 'col'), may hold values from -6 to 6, as said below
- butterfly_scale: float32 [65536], P('row'), may hold values from 0.5 to 2
Outputs:
- transformed: float32 [65536, 4096], P('row', 'col')
The draws below stay inside these ranges and needn't reach their ends.
Inputs may be any that keep to these rules, and one draw needn't show every extreme that they name: The matrix is symmetric where the slab pair meets its own columns: with g(k) = k for k < 2048 and 32768 + k - 2048 otherwise, slab_pair[g(a), b] = slab_pair[g(b), a] for all a, b below 4096.
All inputs are finite; a program needn't handle non-finite values.
Results may differ from the reference program's by a relative error of at most 0.00002.
Values sent between devices are 32-bit elements; how exact they have to be, the bound alone decides.
A program may use at most 64 MiB of HBM per device.

```python
import math
import jax
import jax.numpy as jnp

N = 65536
W = 2048
HALF = 32768


def draw_slab_pair(key, part):
    base = jnp.clip(jax.random.normal(key, (N, 2 * W), jnp.float32), -6.0, 6.0)
    block = jnp.concatenate([base[:W], base[HALF:HALF + W]], axis=0)
    mirrored = jnp.clip((block + block.T) * jnp.float32(0.5) ** 0.5, -6.0, 6.0)
    base = base.at[:W].set(mirrored[:W])
    base = base.at[HALF:HALF + W].set(mirrored[W:])
    return base


def shard_levels(key, dims, pieces, smallest, largest):
    def one(axis_at, parts):
        steps = jax.random.uniform(jax.random.fold_in(jax.random.fold_in(key, 6), axis_at), (parts,), jnp.float32, smallest / len(pieces), largest / len(pieces))
        return jnp.repeat(jnp.exp(steps), dims[axis_at] // parts).reshape((-1,) + (1,) * (len(dims) - axis_at - 1))

    factor_of = one(*pieces[0])
    for cut in pieces[1:]:
        factor_of = factor_of * one(*cut)
    return factor_of


def setup_inputs(seed: int = 0) -> dict:
    arg_keys = jax.random.split(jax.random.key(seed), 3)
    slab_pair = draw_slab_pair(jax.random.fold_in(arg_keys[2], 71), 0)
    butterfly_scale = jnp.clip(jnp.exp(math.log(2.0) - 1.3862944 * jax.random.uniform(arg_keys[1], (N,), jnp.float32) ** shard_levels(arg_keys[1], (N,), ((0, 8),), -0.2, 0.2)), 0.5, 2.0)
    return dict(slab_pair=slab_pair, butterfly_scale=butterfly_scale)


def reference(slab_pair, butterfly_scale):
    root_two = jnp.float32(2.0) ** 0.5
    upper = slab_pair[:HALF]
    lower = slab_pair[HALF:]
    rows_top = butterfly_scale[:HALF, None] * (upper + lower) / root_two
    rows_bottom = butterfly_scale[HALF:, None] * (upper - lower) / root_two
    rows_mixed = jnp.concatenate([rows_top, rows_bottom], axis=0)
    column_scale = jnp.concatenate([butterfly_scale[:W], butterfly_scale[HALF:HALF + W]])
    left_part = rows_mixed[:, :W]
    right_part = rows_mixed[:, W:]
    both_mixed = jnp.concatenate([left_part + right_part, left_part - right_part], axis=1)
    both_mixed = both_mixed * column_scale[None, :] / root_two
    row_index = jnp.arange(N, dtype=jnp.int32)[:, None]
    col_index = jnp.arange(2 * W, dtype=jnp.int32)[None, :]
    global_col = jnp.where(col_index < W, col_index, HALF + col_index - W)
    return jnp.where(row_index >= global_col, both_mixed, jnp.float32(0.0))
```

```python
import functools

import jax
import jax.numpy as jnp
from jax import lax
from jax.experimental import pallas as pl
from jax.experimental.pallas import tpu as pltpu
from jax.sharding import PartitionSpec as P

MESH = pl.DeviceIdType.MESH
N = 65536
W = 2048
CHUNK = 512
LANES = 128


def exchange_kernel(rows, cols, x_ref, s64_ref, s2_ref, out_ref,
                    mid, got1, got2, srow, cscale,
                    load_sem, send1, recv1, send2, recv2, cs_send, cs_recv):
    r = lax.axis_index("row")
    c = lax.axis_index("col")
    local_rows, local_cols = x_ref.shape
    count = local_rows // CHUNK
    half = count // 2
    top = r < rows // 2
    left = c < cols // 2
    z_peer = (lax.rem(r + rows // 2, rows), c)
    x_peer = (r, lax.rem(c + cols // 2, cols))
    source_row = jnp.where(left, 0, rows // 2)
    is_source = r == source_row

    barrier = pltpu.get_barrier_semaphore()
    pl.semaphore_signal(barrier, inc=1, device_id=z_peer, device_id_type=MESH)
    pl.semaphore_signal(barrier, inc=1, device_id=x_peer, device_id_type=MESH)

    @pl.when(jnp.logical_not(is_source))
    def _():
        pl.semaphore_signal(barrier, inc=1, device_id=(source_row, c), device_id_type=MESH)

    def window(i):
        return pl.ds(pl.multiple_of(i * CHUNK, CHUNK), CHUNK)

    def load(i):
        return pltpu.make_async_copy(x_ref.at[window(i)], mid.at[window(i)], load_sem.at[i])

    def first(i, peer):
        return pltpu.make_async_remote_copy(
            x_ref.at[window(i)], got1.at[window(i)], send1.at[i], recv1.at[i],
            device_id=peer, device_id_type=MESH)

    def second(i, peer):
        return pltpu.make_async_remote_copy(
            mid.at[window(i)], got2.at[window(i)], send2.at[i], recv2.at[i],
            device_id=peer, device_id_type=MESH)

    def scales(k):
        return pltpu.make_async_remote_copy(
            s2_ref.at[lax.rem(c, cols // 2)], cscale, cs_send.at[k], cs_recv,
            device_id=(lax.rem(source_row + 1 + k, rows), c), device_id_type=MESH)

    pl.semaphore_wait(barrier, jnp.where(is_source, 2 + rows - 1, 2))

    @pl.loop(0, half)
    def _(i):
        first(i, z_peer).start()
        first(i + half, x_peer).start()

    @pl.loop(0, count)
    def _(i):
        load(i).start()

    @pl.when(is_source)
    def _():
        cscale[...] = s2_ref[lax.rem(c, cols // 2)]

        @pl.loop(0, rows - 1)
        def _(k):
            scales(k).start()

    @pl.loop(0, local_rows // LANES)
    def _(g):
        line = jnp.broadcast_to(s64_ref[pl.ds(g, 1), :], (LANES, LANES))
        srow[pl.ds(pl.multiple_of(g * LANES, LANES), LANES), :] = line.T * jnp.float32(0.5)

    z_sign = jnp.where(top, 1.0, -1.0).astype(jnp.float32)
    x_sign = jnp.where(left, 1.0, -1.0).astype(jnp.float32)

    def mix(i, sign):
        mid[window(i), :] = got1[window(i), :] + sign * mid[window(i), :]

    @pl.loop(0, half)
    def _(i):
        load(i).wait()
        first(i, z_peer).wait_recv()
        mix(i, z_sign)
        second(i, x_peer).start()
        load(i + half).wait()
        first(i + half, x_peer).wait_recv()
        mix(i + half, x_sign)
        second(i + half, z_peer).start()

    @pl.when(is_source)
    def _():
        @pl.loop(0, rows - 1)
        def _(k):
            scales(k).wait_send()

    @pl.when(jnp.logical_not(is_source))
    def _():
        scales(0).wait_recv()

    global_col = jnp.where(left, c * local_cols, N // 2 + c * local_cols - W)

    def finish(i, sign):
        base = r * local_rows + i * CHUNK
        for b in range(local_cols // LANES):
            lanes = slice(b * LANES, (b + 1) * LANES)
            value = got2[window(i), lanes] + sign * mid[window(i), lanes]
            value = value * (srow[window(i), :] * cscale[b : b + 1, :])
            row_index = base + lax.broadcasted_iota(jnp.int32, (CHUNK, LANES), 0)
            col_index = global_col + b * LANES + lax.broadcasted_iota(jnp.int32, (CHUNK, LANES), 1)
            out_ref[window(i), lanes] = jnp.where(row_index >= col_index, value, jnp.float32(0.0))

    @pl.loop(0, half)
    def _(i):
        second(i, x_peer).wait_recv()
        finish(i, x_sign)
        second(i + half, z_peer).wait_recv()
        finish(i + half, z_sign)

    @pl.loop(0, half)
    def _(i):
        first(i, z_peer).wait_send()
        first(i + half, x_peer).wait_send()
        second(i, x_peer).wait_send()
        second(i + half, z_peer).wait_send()


def per_device(rows, cols, slab_pair, butterfly_scale):
    local_rows, local_cols = slab_pair.shape
    count = local_rows // CHUNK
    hbm = pl.BlockSpec(memory_space=pl.ANY)
    vmem = pl.BlockSpec(memory_space=pltpu.VMEM)
    s64 = butterfly_scale.reshape(local_rows // LANES, LANES)
    s2 = butterfly_scale.reshape(local_rows // local_cols, local_cols // LANES, LANES)
    block = pltpu.VMEM((local_rows, local_cols), jnp.float32)
    dma = pltpu.SemaphoreType.DMA
    return pl.pallas_call(
        functools.partial(exchange_kernel, rows, cols),
        out_shape=jax.ShapeDtypeStruct(slab_pair.shape, slab_pair.dtype),
        in_specs=[hbm, vmem, vmem],
        out_specs=vmem,
        scratch_shapes=[
            block, block, block,
            pltpu.VMEM((local_rows, LANES), jnp.float32),
            pltpu.VMEM((local_cols // LANES, LANES), jnp.float32),
            dma((count,)), dma((count,)), dma((count,)), dma((count,)), dma((count,)),
            dma((rows - 1,)), dma,
        ],
        compiler_params=pltpu.CompilerParams(
            collective_id=0, has_side_effects=True, vmem_limit_bytes=40 * 1024 * 1024
        ),
    )(slab_pair, s64, s2)


def solution(mesh):
    return jax.shard_map(
        functools.partial(per_device, mesh.shape["row"], mesh.shape["col"]),
        mesh=mesh,
        in_specs=(P("row", "col"), P("row")),
        out_specs=P("row", "col"),
        check_vma=False,
    )
```

```python
import functools

import jax
import jax.numpy as jnp
from jax import lax
from jax.experimental import pallas as pl
from jax.experimental.pallas import tpu as pltpu
from jax.sharding import PartitionSpec as P

MESH = pl.DeviceIdType.MESH
N = 65536
W = 2048
CHUNK = 256
LANES = 128


def exchange_kernel(rows, cols, x_ref, s64_ref, s2_ref, out_ref,
                    mid, got1, got2, srow, s64, cscale,
                    load_sem, send1, recv1, send2, recv2, cs_send, cs_recv,
                    scale_sem, ready_z, ready_x):
    r = lax.axis_index("row")
    c = lax.axis_index("col")
    local_rows, local_cols = x_ref.shape
    count = local_rows // CHUNK
    half = count // 2
    top = r < rows // 2
    left = c < cols // 2
    z_peer = (lax.rem(r + rows // 2, rows), c)
    x_peer = (r, lax.rem(c + cols // 2, cols))
    source_row = jnp.where(left, 0, rows // 2)
    is_source = r == source_row

    def window(i):
        return pl.ds(pl.multiple_of(i * CHUNK, CHUNK), CHUNK)

    def load(i):
        return pltpu.make_async_copy(x_ref.at[window(i)], mid.at[window(i)], load_sem.at[i])

    def first(i, peer):
        return pltpu.make_async_remote_copy(
            x_ref.at[window(i)], got1.at[window(i)], send1.at[i], recv1.at[i],
            device_id=peer, device_id_type=MESH)

    def second(i, peer):
        return pltpu.make_async_remote_copy(
            mid.at[window(i)], got2.at[window(i)], send2.at[i], recv2.at[i],
            device_id=peer, device_id_type=MESH)

    def scales(k):
        return pltpu.make_async_remote_copy(
            cscale, cscale, cs_send.at[k], cs_recv,
            device_id=(lax.rem(source_row + 1 + k, rows), c), device_id_type=MESH)

    barrier = pltpu.get_barrier_semaphore()

    def greet(peer):
        pl.semaphore_signal(barrier, inc=1, device_id=peer, device_id_type=MESH)

    def answer(ready, peer):
        pl.semaphore_signal(ready, inc=1, device_id=peer, device_id_type=MESH)

    def send_z():
        @pl.loop(0, half)
        def _(i):
            first(i, z_peer).start()

    def send_x():
        @pl.loop(half, count)
        def _(i):
            first(i, x_peer).start()

    @pl.when(top)
    def _():
        greet(z_peer)

    @pl.when(left)
    def _():
        greet(x_peer)

    @pl.when(jnp.logical_not(is_source))
    def _():
        greet((source_row, c))

    greetings = jnp.where(top, 0, 1) + jnp.where(left, 0, 1)

    @pl.when(greetings > 0)
    def _():
        late_source = is_source & jnp.logical_not(left)
        pl.semaphore_wait(barrier, greetings + jnp.where(late_source, rows - 1, 0))

    @pl.when(jnp.logical_not(top))
    def _():
        answer(ready_z, z_peer)
        send_z()

    @pl.when(jnp.logical_not(left))
    def _():
        answer(ready_x, x_peer)
        send_x()

    @pl.when(top)
    def _():
        pl.semaphore_wait(ready_z, 1)
        send_z()

    @pl.when(left)
    def _():
        pl.semaphore_wait(ready_x, 1)
        send_x()

    load_scale = pltpu.make_async_copy(s64_ref, s64, scale_sem.at[0])
    load_scale.start()

    @pl.loop(0, count)
    def _(i):
        load(i).start()

    load_scale.wait()

    @pl.loop(0, local_rows // LANES)
    def _(g):
        line = jnp.broadcast_to(s64[pl.ds(g, 1), :], (LANES, LANES))
        srow[pl.ds(pl.multiple_of(g * LANES, LANES), LANES), :] = line.T * jnp.float32(0.5)

    own_scale = pltpu.make_async_copy(s2_ref.at[lax.rem(c, cols // 2)], cscale, scale_sem.at[1])

    @pl.when(is_source)
    def _():
        own_scale.start()
        own_scale.wait()

        @pl.when(left)
        def _():
            pl.semaphore_wait(barrier, rows - 1)

        @pl.loop(0, rows - 1)
        def _(k):
            scales(k).start()

    z_sign = jnp.where(top, 1.0, -1.0).astype(jnp.float32)
    x_sign = jnp.where(left, 1.0, -1.0).astype(jnp.float32)

    def mix(i, sign):
        mid[window(i), :] = got1[window(i), :] + sign * mid[window(i), :]

    @pl.loop(0, half)
    def _(i):
        load(i).wait()
        first(i, z_peer).wait_recv()
        mix(i, z_sign)
        second(i, x_peer).start()
        load(i + half).wait()
        first(i + half, x_peer).wait_recv()
        mix(i + half, x_sign)
        second(i + half, z_peer).start()

    @pl.when(is_source)
    def _():
        @pl.loop(0, rows - 1)
        def _(k):
            scales(k).wait_send()

    @pl.when(jnp.logical_not(is_source))
    def _():
        scales(0).wait_recv()

    global_col = jnp.where(left, c * local_cols, N // 2 + c * local_cols - W)

    def finish(i, sign):
        base = r * local_rows + i * CHUNK
        for b in range(local_cols // LANES):
            lanes = slice(b * LANES, (b + 1) * LANES)
            value = got2[window(i), lanes] + sign * mid[window(i), lanes]
            value = value * (srow[window(i), :] * cscale[b : b + 1, :])
            row_index = base + lax.broadcasted_iota(jnp.int32, (CHUNK, LANES), 0)
            col_index = global_col + b * LANES + lax.broadcasted_iota(jnp.int32, (CHUNK, LANES), 1)
            out_ref[window(i), lanes] = jnp.where(row_index >= col_index, value, jnp.float32(0.0))

    @pl.loop(0, half)
    def _(i):
        second(i, x_peer).wait_recv()
        finish(i, x_sign)
        second(i + half, z_peer).wait_recv()
        finish(i + half, z_sign)

    @pl.loop(0, half)
    def _(i):
        first(i, z_peer).wait_send()
        first(i + half, x_peer).wait_send()
        second(i, x_peer).wait_send()
        second(i + half, z_peer).wait_send()


def per_device(rows, cols, slab_pair, butterfly_scale):
    local_rows, local_cols = slab_pair.shape
    count = local_rows // CHUNK
    hbm = pl.BlockSpec(memory_space=pltpu.HBM)
    vmem = pl.BlockSpec(memory_space=pltpu.VMEM)
    s64 = butterfly_scale.reshape(local_rows // LANES, LANES)
    s2 = butterfly_scale.reshape(local_rows // local_cols, local_cols // LANES, LANES)
    block = pltpu.VMEM((local_rows, local_cols), jnp.float32)
    dma = pltpu.SemaphoreType.DMA
    return pl.pallas_call(
        functools.partial(exchange_kernel, rows, cols),
        out_shape=jax.ShapeDtypeStruct(slab_pair.shape, slab_pair.dtype),
        in_specs=[hbm, hbm, hbm],
        out_specs=vmem,
        scratch_shapes=[
            block, block, block,
            pltpu.VMEM((local_rows, LANES), jnp.float32),
            pltpu.VMEM((local_rows // LANES, LANES), jnp.float32),
            pltpu.VMEM((local_cols // LANES, LANES), jnp.float32),
            dma((count,)), dma((count,)), dma((count,)), dma((count,)), dma((count,)),
            dma((rows - 1,)), dma, dma((2,)),
            pltpu.SemaphoreType.REGULAR, pltpu.SemaphoreType.REGULAR,
        ],
        compiler_params=pltpu.CompilerParams(
            collective_id=0, has_side_effects=True, vmem_limit_bytes=40 * 1024 * 1024
        ),
    )(slab_pair, *(pltpu.with_memory_space_constraint(s, pltpu.HBM) for s in (s64, s2)))


def solution(mesh):
    return jax.shard_map(
        functools.partial(per_device, mesh.shape["row"], mesh.shape["col"]),
        mesh=mesh,
        in_specs=(P("row", "col"), P("row")),
        out_specs=P("row", "col"),
        check_vma=False,
    )
```

```python
import functools

import jax
import jax.numpy as jnp
from jax import lax
from jax.experimental import pallas as pl
from jax.experimental.pallas import tpu as pltpu
from jax.sharding import PartitionSpec as P

MESH = pl.DeviceIdType.MESH
N = 65536
W = 2048
FIRST = (2048, 2048)
SECOND = (2048, 1024, 512, 256, 256)
STEP = 256
LANES = 128


def spans(sizes, base):
    out = []
    for size in sizes:
        out.append((base, size))
        base += size
    return out


def exchange_kernel(rows, cols, x_ref, s64_ref, s2_ref, out_ref,
                    mid, got1, got2, srow, s64, cscale,
                    load_sem, send1, recv1, send2, recv2, cs_send, cs_recv,
                    scale_sem, ready_z, ready_x):
    r = lax.axis_index("row")
    c = lax.axis_index("col")
    local_rows, local_cols = x_ref.shape
    half_rows = local_rows // 2
    pieces1 = spans(FIRST, 0), spans(FIRST, half_rows)
    pieces2 = spans(SECOND, 0), spans(SECOND, half_rows)
    top = r < rows // 2
    left = c < cols // 2
    z_peer = (lax.rem(r + rows // 2, rows), c)
    x_peer = (r, lax.rem(c + cols // 2, cols))
    source_row = jnp.where(left, 0, rows // 2)
    is_source = r == source_row

    def load(half, i):
        window = pl.ds(*pieces1[half][i])
        return pltpu.make_async_copy(x_ref.at[window], mid.at[window], load_sem.at[half, i])

    def first(half, i):
        window = pl.ds(*pieces1[half][i])
        return pltpu.make_async_remote_copy(
            x_ref.at[window], got1.at[window], send1.at[half, i], recv1.at[half, i],
            device_id=(z_peer, x_peer)[half], device_id_type=MESH)

    def second(half, i):
        window = pl.ds(*pieces2[half][i])
        return pltpu.make_async_remote_copy(
            mid.at[window], got2.at[window], send2.at[half, i], recv2.at[half, i],
            device_id=(x_peer, z_peer)[half], device_id_type=MESH)

    def scales(k):
        return pltpu.make_async_remote_copy(
            cscale, cscale, cs_send.at[k], cs_recv,
            device_id=(lax.rem(source_row + 1 + k, rows), c), device_id_type=MESH)

    barrier = pltpu.get_barrier_semaphore()

    def greet(peer):
        pl.semaphore_signal(barrier, inc=1, device_id=peer, device_id_type=MESH)

    def answer(ready, peer):
        pl.semaphore_signal(ready, inc=1, device_id=peer, device_id_type=MESH)

    def send_z():
        for i in range(len(FIRST)):
            first(0, i).start()

    def send_x():
        for i in range(len(FIRST)):
            first(1, i).start()

    @pl.when(top)
    def _():
        greet(z_peer)

    @pl.when(left)
    def _():
        greet(x_peer)

    @pl.when(jnp.logical_not(is_source))
    def _():
        greet((source_row, c))

    greetings = jnp.where(top, 0, 1) + jnp.where(left, 0, 1)

    @pl.when(greetings > 0)
    def _():
        late_source = is_source & jnp.logical_not(left)
        pl.semaphore_wait(barrier, greetings + jnp.where(late_source, rows - 1, 0))

    @pl.when(jnp.logical_not(top))
    def _():
        answer(ready_z, z_peer)
        send_z()

    @pl.when(jnp.logical_not(left))
    def _():
        answer(ready_x, x_peer)
        send_x()

    @pl.when(top)
    def _():
        pl.semaphore_wait(ready_z, 1)
        send_z()

    @pl.when(left)
    def _():
        pl.semaphore_wait(ready_x, 1)
        send_x()

    load_scale = pltpu.make_async_copy(s64_ref, s64, scale_sem.at[0])
    load_scale.start()

    for i in range(len(FIRST)):
        load(0, i).start()
        load(1, i).start()

    load_scale.wait()

    @pl.loop(0, local_rows // LANES)
    def _(g):
        line = jnp.broadcast_to(s64[pl.ds(g, 1), :], (LANES, LANES))
        srow[pl.ds(pl.multiple_of(g * LANES, LANES), LANES), :] = line.T * jnp.float32(0.5)

    own_scale = pltpu.make_async_copy(s2_ref.at[lax.rem(c, cols // 2)], cscale, scale_sem.at[1])

    @pl.when(is_source)
    def _():
        own_scale.start()
        own_scale.wait()

        @pl.when(left)
        def _():
            pl.semaphore_wait(barrier, rows - 1)

        @pl.loop(0, rows - 1)
        def _(k):
            scales(k).start()

    z_sign = jnp.where(top, 1.0, -1.0).astype(jnp.float32)
    x_sign = jnp.where(left, 1.0, -1.0).astype(jnp.float32)

    first_sign = z_sign, x_sign
    second_sign = x_sign, z_sign

    for i in range(len(FIRST)):
        for half in range(2):
            base, size = pieces1[half][i]
            load(half, i).wait()
            first(half, i).wait_recv()

            @pl.loop(0, size // STEP)
            def _(t):
                window = pl.ds(pl.multiple_of(base + t * STEP, STEP), STEP)
                mid[window, :] = got1[window, :] + first_sign[half] * mid[window, :]

            for j, (start, length) in enumerate(pieces2[half]):
                if base < start + length <= base + size:
                    second(half, j).start()

    @pl.when(is_source)
    def _():
        @pl.loop(0, rows - 1)
        def _(k):
            scales(k).wait_send()

    @pl.when(jnp.logical_not(is_source))
    def _():
        scales(0).wait_recv()

    global_col = jnp.where(left, c * local_cols, N // 2 + c * local_cols - W)

    for i in range(len(SECOND)):
        for half in range(2):
            base, size = pieces2[half][i]
            second(half, i).wait_recv()

            @pl.loop(0, size // STEP)
            def _(t):
                here = base + t * STEP
                window = pl.ds(pl.multiple_of(here, STEP), STEP)
                for b in range(local_cols // LANES):
                    lanes = slice(b * LANES, (b + 1) * LANES)
                    value = got2[window, lanes] + second_sign[half] * mid[window, lanes]
                    value = value * (srow[window, :] * cscale[b : b + 1, :])
                    row_index = r * local_rows + here + lax.broadcasted_iota(jnp.int32, value.shape, 0)
                    col_index = global_col + b * LANES + lax.broadcasted_iota(jnp.int32, value.shape, 1)
                    out_ref[window, lanes] = jnp.where(row_index >= col_index, value, jnp.float32(0.0))

    for half in range(2):
        for i in range(len(FIRST)):
            first(half, i).wait_send()
        for i in range(len(SECOND)):
            second(half, i).wait_send()


def per_device(rows, cols, slab_pair, butterfly_scale):
    local_rows, local_cols = slab_pair.shape
    hbm = pl.BlockSpec(memory_space=pltpu.HBM)
    vmem = pl.BlockSpec(memory_space=pltpu.VMEM)
    s64 = butterfly_scale.reshape(local_rows // LANES, LANES)
    s2 = butterfly_scale.reshape(local_rows // local_cols, local_cols // LANES, LANES)
    block = pltpu.VMEM((local_rows, local_cols), jnp.float32)
    dma = pltpu.SemaphoreType.DMA
    return pl.pallas_call(
        functools.partial(exchange_kernel, rows, cols),
        out_shape=jax.ShapeDtypeStruct(slab_pair.shape, slab_pair.dtype),
        in_specs=[hbm, hbm, hbm],
        out_specs=vmem,
        scratch_shapes=[
            block, block, block,
            pltpu.VMEM((local_rows, LANES), jnp.float32),
            pltpu.VMEM((local_rows // LANES, LANES), jnp.float32),
            pltpu.VMEM((local_cols // LANES, LANES), jnp.float32),
            dma((2, len(FIRST))), dma((2, len(FIRST))), dma((2, len(FIRST))),
            dma((2, len(SECOND))), dma((2, len(SECOND))),
            dma((rows - 1,)), dma, dma((2,)),
            pltpu.SemaphoreType.REGULAR, pltpu.SemaphoreType.REGULAR,
        ],
        compiler_params=pltpu.CompilerParams(
            collective_id=0, has_side_effects=True, vmem_limit_bytes=40 * 1024 * 1024
        ),
    )(slab_pair, *(pltpu.with_memory_space_constraint(s, pltpu.HBM) for s in (s64, s2)))


def solution(mesh):
    return jax.shard_map(
        functools.partial(per_device, mesh.shape["row"], mesh.shape["col"]),
        mesh=mesh,
        in_specs=(P("row", "col"), P("row")),
        out_specs=P("row", "col"),
        check_vma=False,
    )
```

```python
import functools

import jax
import jax.numpy as jnp
from jax import lax
from jax.experimental import pallas as pl
from jax.experimental.pallas import tpu as pltpu
from jax.sharding import PartitionSpec as P

MESH = pl.DeviceIdType.MESH
N = 65536
W = 2048
FIRST = (2048, 2048)
SECOND = (2048, 1024, 512, 256, 256)
STEP = 256
LANES = 128


def spans(sizes, base):
    out = []
    for size in sizes:
        out.append((base, size))
        base += size
    return out


def exchange_kernel(rows, cols, x_ref, s64_ref, s2_ref, out_ref,
                    mid, got1, got2, srow, s64, cscale,
                    load_sem, send1, recv1, send2, recv2, cs_send, cs_recv,
                    scale_sem, ready_z, ready_x, all_in):
    r = lax.axis_index("row")
    c = lax.axis_index("col")
    local_rows, local_cols = x_ref.shape
    half_rows = local_rows // 2
    pieces1 = spans(FIRST, 0), spans(FIRST, half_rows)
    pieces2 = spans(SECOND, 0), spans(SECOND, half_rows)
    top = r < rows // 2
    left = c < cols // 2
    z_peer = (lax.rem(r + rows // 2, rows), c)
    x_peer = (r, lax.rem(c + cols // 2, cols))
    half_cols = cols // 2
    source_row = jnp.where(left, 0, rows // 2)
    is_source = r == source_row
    hub = is_source & left

    def load(half, i):
        window = pl.ds(*pieces1[half][i])
        return pltpu.make_async_copy(x_ref.at[window], mid.at[window], load_sem.at[half])

    def first(half, i):
        window = pl.ds(*pieces1[half][i])
        return pltpu.make_async_remote_copy(
            x_ref.at[window], got1.at[window], send1.at[half], recv1.at[half, i],
            device_id=(z_peer, x_peer)[half], device_id_type=MESH)

    def second(half, i):
        window = pl.ds(*pieces2[half][i])
        return pltpu.make_async_remote_copy(
            mid.at[window], got2.at[window], send2.at[half], recv2.at[half, i],
            device_id=(x_peer, z_peer)[half], device_id_type=MESH)

    def scales(k):
        return pltpu.make_async_remote_copy(
            cscale, cscale, cs_send.at[k], cs_recv,
            device_id=(lax.rem(source_row + 1 + k, rows), c), device_id_type=MESH)

    barrier = pltpu.get_barrier_semaphore()

    def greet(peer):
        pl.semaphore_signal(barrier, inc=1, device_id=peer, device_id_type=MESH)

    def answer(ready, peer):
        pl.semaphore_signal(ready, inc=1, device_id=peer, device_id_type=MESH)

    def send_z():
        for i in range(len(FIRST)):
            first(0, i).start()

    def send_x():
        for i in range(len(FIRST)):
            first(1, i).start()

    @pl.when(top)
    def _():
        greet(z_peer)

    @pl.when(left)
    def _():
        greet(x_peer)

    @pl.when(jnp.logical_not(hub))
    def _():
        greet((0, lax.rem(c, half_cols)))

    greetings = jnp.where(top, 0, 1) + jnp.where(left, 0, 1)

    @pl.when(greetings > 0)
    def _():
        pl.semaphore_wait(barrier, greetings)

    @pl.when(jnp.logical_not(top))
    def _():
        answer(ready_z, z_peer)
        send_z()

    @pl.when(jnp.logical_not(left))
    def _():
        answer(ready_x, x_peer)
        send_x()

    @pl.when(top)
    def _():
        pl.semaphore_wait(ready_z, 1)
        send_z()

    @pl.when(left)
    def _():
        pl.semaphore_wait(ready_x, 1)
        send_x()

    load_scale = pltpu.make_async_copy(s64_ref, s64, scale_sem.at[0])
    load_scale.start()

    for i in range(len(FIRST)):
        load(0, i).start()
        load(1, i).start()

    load_scale.wait()

    @pl.loop(0, local_rows // LANES)
    def _(g):
        line = jnp.broadcast_to(s64[pl.ds(g, 1), :], (LANES, LANES))
        srow[pl.ds(pl.multiple_of(g * LANES, LANES), LANES), :] = line.T * jnp.float32(0.5)

    @pl.when(hub)
    def _():
        pl.semaphore_wait(barrier, 2 * rows - 1)
        answer(all_in, (rows // 2, c + half_cols))

    @pl.when(is_source)
    def _():
        own_scale = pltpu.make_async_copy(s2_ref.at[lax.rem(c, half_cols)], cscale, scale_sem.at[1])
        own_scale.start()
        own_scale.wait()

        @pl.when(jnp.logical_not(left))
        def _():
            pl.semaphore_wait(all_in, 1)

        @pl.loop(0, rows - 1)
        def _(k):
            scales(k).start()

    z_sign = jnp.where(top, 1.0, -1.0).astype(jnp.float32)
    x_sign = jnp.where(left, 1.0, -1.0).astype(jnp.float32)

    first_sign = z_sign, x_sign
    second_sign = x_sign, z_sign

    for i in range(len(FIRST)):
        for half in range(2):
            base, size = pieces1[half][i]
            if i == 0:
                whole = pl.ds(half * half_rows, half_rows)
                pltpu.make_async_copy(x_ref.at[whole], mid.at[whole], load_sem.at[half]).wait()
            first(half, i).wait_recv()

            @pl.loop(0, size // STEP)
            def _(t):
                window = pl.ds(pl.multiple_of(base + t * STEP, STEP), STEP)
                mid[window, :] = got1[window, :] + first_sign[half] * mid[window, :]

            for j, (start, length) in enumerate(pieces2[half]):
                if base < start + length <= base + size:
                    second(half, j).start()

    @pl.when(is_source)
    def _():
        @pl.loop(0, rows - 1)
        def _(k):
            scales(k).wait_send()

    @pl.when(jnp.logical_not(is_source))
    def _():
        scales(0).wait_recv()

    global_col = jnp.where(left, c * local_cols, N // 2 + c * local_cols - W)

    for i in range(len(SECOND)):
        for half in range(2):
            base, size = pieces2[half][i]
            second(half, i).wait_recv()

            @pl.loop(0, size // STEP)
            def _(t):
                here = base + t * STEP
                window = pl.ds(pl.multiple_of(here, STEP), STEP)
                for b in range(local_cols // LANES):
                    lanes = slice(b * LANES, (b + 1) * LANES)
                    value = got2[window, lanes] + second_sign[half] * mid[window, lanes]
                    value = value * (srow[window, :] * cscale[b : b + 1, :])
                    row_index = r * local_rows + here + lax.broadcasted_iota(jnp.int32, value.shape, 0)
                    col_index = global_col + b * LANES + lax.broadcasted_iota(jnp.int32, value.shape, 1)
                    out_ref[window, lanes] = jnp.where(row_index >= col_index, value, jnp.float32(0.0))

    for half in range(2):
        whole = pl.ds(half * half_rows, half_rows)
        for source, sem, peer in ((x_ref, send1, (z_peer, x_peer)), (mid, send2, (x_peer, z_peer))):
            pltpu.make_async_remote_copy(
                source.at[whole], got1.at[whole], sem.at[half], recv1.at[half, 0],
                device_id=peer[half], device_id_type=MESH).wait_send()


def per_device(rows, cols, slab_pair, butterfly_scale):
    local_rows, local_cols = slab_pair.shape
    hbm = pl.BlockSpec(memory_space=pltpu.HBM)
    vmem = pl.BlockSpec(memory_space=pltpu.VMEM)
    s64 = butterfly_scale.reshape(local_rows // LANES, LANES)
    s2 = butterfly_scale.reshape(local_rows // local_cols, local_cols // LANES, LANES)
    block = pltpu.VMEM((local_rows, local_cols), jnp.float32)
    dma = pltpu.SemaphoreType.DMA
    return pl.pallas_call(
        functools.partial(exchange_kernel, rows, cols),
        out_shape=jax.ShapeDtypeStruct(slab_pair.shape, slab_pair.dtype),
        in_specs=[hbm, hbm, hbm],
        out_specs=vmem,
        scratch_shapes=[
            block, block, block,
            pltpu.VMEM((local_rows, LANES), jnp.float32),
            pltpu.VMEM((local_rows // LANES, LANES), jnp.float32),
            pltpu.VMEM((local_cols // LANES, LANES), jnp.float32),
            dma((2,)), dma((2,)), dma((2, len(FIRST))), dma((2,)), dma((2, len(SECOND))),
            dma((rows - 1,)), dma, dma((2,)),
            pltpu.SemaphoreType.REGULAR, pltpu.SemaphoreType.REGULAR, pltpu.SemaphoreType.REGULAR,
        ],
        compiler_params=pltpu.CompilerParams(
            collective_id=0, has_side_effects=True, vmem_limit_bytes=40 * 1024 * 1024
        ),
    )(slab_pair, *(pltpu.with_memory_space_constraint(s, pltpu.HBM) for s in (s64, s2)))


def solution(mesh):
    return jax.shard_map(
        functools.partial(per_device, mesh.shape["row"], mesh.shape["col"]),
        mesh=mesh,
        in_specs=(P("row", "col"), P("row")),
        out_specs=P("row", "col"),
        check_vma=False,
    )
```

```python
import functools

import jax
import jax.numpy as jnp
from jax import lax
from jax.experimental import pallas as pl
from jax.experimental.pallas import tpu as pltpu
from jax.sharding import PartitionSpec as P

MESH = pl.DeviceIdType.MESH
N = 65536
W = 2048
FIRST = (256, 1792, 2048)
SECOND = (2048, 1024, 512, 256, 256)
STEP = 256
LANES = 128


def spans(sizes, base):
    out = []
    for size in sizes:
        out.append((base, size))
        base += size
    return out


def exchange_kernel(rows, cols, x_ref, s64_ref, s2_ref, out_ref,
                    mid, got1, got2, srow, s64, cscale,
                    load_sem, send1, recv1, send2, recv2, cs_send, cs_recv,
                    scale_sem, ready_z, ready_x, all_in):
    r = lax.axis_index("row")
    c = lax.axis_index("col")
    local_rows, local_cols = x_ref.shape
    half_rows = local_rows // 2
    pieces1 = spans(FIRST, 0), spans(FIRST, half_rows)
    pieces2 = spans(SECOND, 0), spans(SECOND, half_rows)
    top = r < rows // 2
    left = c < cols // 2
    z_peer = (lax.rem(r + rows // 2, rows), c)
    x_peer = (r, lax.rem(c + cols // 2, cols))
    half_cols = cols // 2
    source_row = jnp.where(left, 0, rows // 2)
    is_source = r == source_row
    hub = is_source & left

    def load(half, i):
        window = pl.ds(*pieces1[half][i])
        return pltpu.make_async_copy(x_ref.at[window], mid.at[window], load_sem.at[half, i])

    def first(half, i):
        window = pl.ds(*pieces1[half][i])
        return pltpu.make_async_remote_copy(
            (x_ref if i else mid).at[window], got1.at[window],
            send1.at[half, min(i, 1)], recv1.at[half, i],
            device_id=(z_peer, x_peer)[half], device_id_type=MESH)

    def second(half, i):
        window = pl.ds(*pieces2[half][i])
        return pltpu.make_async_remote_copy(
            mid.at[window], got2.at[window], send2.at[half], recv2.at[half, i],
            device_id=(x_peer, z_peer)[half], device_id_type=MESH)

    def scales(k):
        return pltpu.make_async_remote_copy(
            cscale, cscale, cs_send.at[k], cs_recv,
            device_id=(lax.rem(source_row + 1 + k, rows), c), device_id_type=MESH)

    barrier = pltpu.get_barrier_semaphore()

    def greet(peer):
        pl.semaphore_signal(barrier, inc=1, device_id=peer, device_id_type=MESH)

    def answer(ready, peer):
        pl.semaphore_signal(ready, inc=1, device_id=peer, device_id_type=MESH)

    def send_z():
        load(0, 0).wait()
        for i in range(len(FIRST)):
            first(0, i).start()

    def send_x():
        load(1, 0).wait()
        for i in range(len(FIRST)):
            first(1, i).start()

    load(0, 0).start()
    load(1, 0).start()

    @pl.when(top)
    def _():
        greet(z_peer)

    @pl.when(left)
    def _():
        greet(x_peer)

    @pl.when(jnp.logical_not(hub))
    def _():
        greet((0, lax.rem(c, half_cols)))

    greetings = jnp.where(top, 0, 1) + jnp.where(left, 0, 1)

    @pl.when(greetings > 0)
    def _():
        pl.semaphore_wait(barrier, greetings)

    @pl.when(jnp.logical_not(top))
    def _():
        answer(ready_z, z_peer)

    @pl.when(jnp.logical_not(left))
    def _():
        answer(ready_x, x_peer)
        send_x()

    @pl.when(jnp.logical_not(top))
    def _():
        send_z()

    @pl.when(top)
    def _():
        pl.semaphore_wait(ready_z, 1)
        send_z()

    @pl.when(left)
    def _():
        pl.semaphore_wait(ready_x, 1)
        send_x()

    load_scale = pltpu.make_async_copy(s64_ref, s64, scale_sem.at[0])
    load_scale.start()

    for i in range(1, len(FIRST)):
        load(0, i).start()
        load(1, i).start()

    load_scale.wait()

    @pl.loop(0, local_rows // LANES)
    def _(g):
        line = jnp.broadcast_to(s64[pl.ds(g, 1), :], (LANES, LANES))
        srow[pl.ds(pl.multiple_of(g * LANES, LANES), LANES), :] = line.T * jnp.float32(0.5)

    @pl.when(hub)
    def _():
        pl.semaphore_wait(barrier, 2 * rows - 1)
        answer(all_in, (rows // 2, c + half_cols))

    @pl.when(is_source)
    def _():
        own_scale = pltpu.make_async_copy(s2_ref.at[lax.rem(c, half_cols)], cscale, scale_sem.at[1])
        own_scale.start()
        own_scale.wait()

        @pl.when(jnp.logical_not(left))
        def _():
            pl.semaphore_wait(all_in, 1)

        @pl.loop(0, rows - 1)
        def _(k):
            scales(k).start()

    z_sign = jnp.where(top, 1.0, -1.0).astype(jnp.float32)
    x_sign = jnp.where(left, 1.0, -1.0).astype(jnp.float32)

    blank = top & jnp.logical_not(left)
    needed = jnp.logical_not(top & left), top | left
    first_sign = z_sign, x_sign
    second_sign = x_sign, z_sign

    for i in range(len(FIRST)):
        for half in range(2):
            base, size = pieces1[half][i]
            first(half, i).wait_recv()
            if i:
                load(half, i).wait()
            else:
                first(half, i).wait_send()

            @pl.loop(0, size // STEP)
            def _(t):
                window = pl.ds(pl.multiple_of(base + t * STEP, STEP), STEP)
                mid[window, :] = got1[window, :] + first_sign[half] * mid[window, :]

            @pl.when(needed[half])
            def _():
                for j, (start, length) in enumerate(pieces2[half]):
                    if base < start + length <= base + size:
                        second(half, j).start()

    @pl.when(is_source)
    def _():
        @pl.loop(0, rows - 1)
        def _(k):
            scales(k).wait_send()

    @pl.when(jnp.logical_not(is_source))
    def _():
        scales(0).wait_recv()

    global_col = jnp.where(left, c * local_cols, N // 2 + c * local_cols - W)

    @pl.when(blank)
    def _():
        @pl.loop(0, local_rows // STEP)
        def _(t):
            out_ref[pl.ds(pl.multiple_of(t * STEP, STEP), STEP), :] = jnp.zeros((STEP, local_cols), jnp.float32)

    @pl.when(jnp.logical_not(blank))
    def _():
        for i in range(len(SECOND)):
            for half in range(2):
                base, size = pieces2[half][i]
                second(half, i).wait_recv()

                @pl.loop(0, size // STEP)
                def _(t):
                    here = base + t * STEP
                    window = pl.ds(pl.multiple_of(here, STEP), STEP)
                    for b in range(local_cols // LANES):
                        lanes = slice(b * LANES, (b + 1) * LANES)
                        value = got2[window, lanes] + second_sign[half] * mid[window, lanes]
                        value = value * (srow[window, :] * cscale[b : b + 1, :])
                        row_index = r * local_rows + here + lax.broadcasted_iota(jnp.int32, value.shape, 0)
                        col_index = global_col + b * LANES + lax.broadcasted_iota(jnp.int32, value.shape, 1)
                        out_ref[window, lanes] = jnp.where(row_index >= col_index, value, jnp.float32(0.0))

    def drained(source, base, size, sem):
        window = pl.ds(base, size)
        pltpu.make_async_remote_copy(
            source.at[window], got1.at[window], sem, recv1.at[0, 0],
            device_id=z_peer, device_id_type=MESH).wait_send()

    for half in range(2):
        drained(x_ref, half * half_rows + FIRST[0], half_rows - FIRST[0], send1.at[half, 1])

        @pl.when(needed[half])
        def _():
            drained(mid, half * half_rows, half_rows, send2.at[half])


def per_device(rows, cols, slab_pair, butterfly_scale):
    local_rows, local_cols = slab_pair.shape
    hbm = pl.BlockSpec(memory_space=pltpu.HBM)
    vmem = pl.BlockSpec(memory_space=pltpu.VMEM)
    s64 = butterfly_scale.reshape(local_rows // LANES, LANES)
    s2 = butterfly_scale.reshape(local_rows // local_cols, local_cols // LANES, LANES)
    block = pltpu.VMEM((local_rows, local_cols), jnp.float32)
    dma = pltpu.SemaphoreType.DMA
    return pl.pallas_call(
        functools.partial(exchange_kernel, rows, cols),
        out_shape=jax.ShapeDtypeStruct(slab_pair.shape, slab_pair.dtype),
        in_specs=[hbm, hbm, hbm],
        out_specs=vmem,
        scratch_shapes=[
            block, block, block,
            pltpu.VMEM((local_rows, LANES), jnp.float32),
            pltpu.VMEM((local_rows // LANES, LANES), jnp.float32),
            pltpu.VMEM((local_cols // LANES, LANES), jnp.float32),
            dma((2, len(FIRST))), dma((2, 2)), dma((2, len(FIRST))), dma((2,)), dma((2, len(SECOND))),
            dma((rows - 1,)), dma, dma((2,)),
            pltpu.SemaphoreType.REGULAR, pltpu.SemaphoreType.REGULAR, pltpu.SemaphoreType.REGULAR,
        ],
        compiler_params=pltpu.CompilerParams(
            collective_id=0, has_side_effects=True, vmem_limit_bytes=40 * 1024 * 1024
        ),
    )(slab_pair, *(pltpu.with_memory_space_constraint(s, pltpu.HBM) for s in (s64, s2)))


def solution(mesh):
    return jax.shard_map(
        functools.partial(per_device, mesh.shape["row"], mesh.shape["col"]),
        mesh=mesh,
        in_specs=(P("row", "col"), P("row")),
        out_specs=P("row", "col"),
        check_vma=False,
    )
```

```python
import functools

import jax
import jax.numpy as jnp
from jax import lax
from jax.experimental import pallas as pl
from jax.experimental.pallas import tpu as pltpu
from jax.sharding import PartitionSpec as P

MESH = pl.DeviceIdType.MESH
N = 65536
W = 2048
FIRST = (128, 1920, 2048)
SECOND = (2048, 1536, 384, 128)
STEP = 128
LANES = 128


def spans(sizes, base):
    out = []
    for size in sizes:
        out.append((base, size))
        base += size
    return out


def exchange_kernel(rows, cols, x_ref, s64_ref, s2_ref, out_ref,
                    mid, got1, got2, srow, s64, cscale,
                    load_sem, send1, recv1, send2, recv2, cs_send, cs_recv,
                    scale_sem, ready_z, ready_x, all_in):
    r = lax.axis_index("row")
    c = lax.axis_index("col")
    local_rows, local_cols = x_ref.shape
    half_rows = local_rows // 2
    pieces1 = spans(FIRST, 0), spans(FIRST, half_rows)
    pieces2 = spans(SECOND, 0), spans(SECOND, half_rows)
    top = r < rows // 2
    left = c < cols // 2
    z_peer = (lax.rem(r + rows // 2, rows), c)
    x_peer = (r, lax.rem(c + cols // 2, cols))
    half_cols = cols // 2
    source_row = jnp.where(left, 0, rows // 2)
    is_source = r == source_row
    hub = is_source & left

    def load(half, i):
        window = pl.ds(*pieces1[half][i])
        return pltpu.make_async_copy(x_ref.at[window], mid.at[window], load_sem.at[half, i])

    def first(half, i):
        window = pl.ds(*pieces1[half][i])
        return pltpu.make_async_remote_copy(
            (x_ref if i else mid).at[window], got1.at[window],
            send1.at[half, min(i, 1)], recv1.at[half, i],
            device_id=(z_peer, x_peer)[half], device_id_type=MESH)

    def second(half, i):
        window = pl.ds(*pieces2[half][i])
        return pltpu.make_async_remote_copy(
            mid.at[window], got2.at[window], send2.at[half], recv2.at[half, i],
            device_id=(x_peer, z_peer)[half], device_id_type=MESH)

    def scales(k):
        return pltpu.make_async_remote_copy(
            cscale, cscale, cs_send.at[k], cs_recv,
            device_id=(lax.rem(source_row + 1 + k, rows), c), device_id_type=MESH)

    barrier = pltpu.get_barrier_semaphore()

    def greet(peer):
        pl.semaphore_signal(barrier, inc=1, device_id=peer, device_id_type=MESH)

    def answer(ready, peer):
        pl.semaphore_signal(ready, inc=1, device_id=peer, device_id_type=MESH)

    def send_z():
        load(0, 0).wait()
        for i in range(len(FIRST)):
            first(0, i).start()

    def send_x():
        load(1, 0).wait()
        for i in range(len(FIRST)):
            first(1, i).start()

    load(0, 0).start()
    load(1, 0).start()

    @pl.when(top)
    def _():
        greet(z_peer)

    @pl.when(left)
    def _():
        greet(x_peer)

    @pl.when(jnp.logical_not(hub))
    def _():
        greet((0, lax.rem(c, half_cols)))

    greetings = jnp.where(top, 0, 1) + jnp.where(left, 0, 1)

    @pl.when(greetings > 0)
    def _():
        pl.semaphore_wait(barrier, greetings)

    @pl.when(jnp.logical_not(top))
    def _():
        answer(ready_z, z_peer)

    @pl.when(jnp.logical_not(left))
    def _():
        answer(ready_x, x_peer)
        send_x()

    @pl.when(jnp.logical_not(top))
    def _():
        send_z()

    @pl.when(top)
    def _():
        pl.semaphore_wait(ready_z, 1)
        send_z()

    @pl.when(left)
    def _():
        pl.semaphore_wait(ready_x, 1)
        send_x()

    load_scale = pltpu.make_async_copy(s64_ref, s64, scale_sem.at[0])
    load_scale.start()

    for i in range(1, len(FIRST)):
        load(0, i).start()
        load(1, i).start()

    load_scale.wait()

    @pl.loop(0, local_rows // LANES)
    def _(g):
        line = jnp.broadcast_to(s64[pl.ds(g, 1), :], (LANES, LANES))
        srow[pl.ds(pl.multiple_of(g * LANES, LANES), LANES), :] = line.T * jnp.float32(0.5)

    @pl.when(hub)
    def _():
        pl.semaphore_wait(barrier, 2 * rows - 1)
        answer(all_in, (rows // 2, c + half_cols))

    @pl.when(is_source)
    def _():
        own_scale = pltpu.make_async_copy(s2_ref.at[lax.rem(c, half_cols)], cscale, scale_sem.at[1])
        own_scale.start()
        own_scale.wait()

        @pl.when(jnp.logical_not(left))
        def _():
            pl.semaphore_wait(all_in, 1)

        @pl.loop(0, rows - 1)
        def _(k):
            scales(k).start()

    z_sign = jnp.where(top, 1.0, -1.0).astype(jnp.float32)
    x_sign = jnp.where(left, 1.0, -1.0).astype(jnp.float32)

    first_sign = z_sign, x_sign
    second_sign = x_sign, z_sign

    for i in range(len(FIRST)):
        for half in range(2):
            base, size = pieces1[half][i]
            first(half, i).wait_recv()
            if i:
                load(half, i).wait()
            else:
                first(half, i).wait_send()

            @pl.loop(0, size // STEP)
            def _(t):
                window = pl.ds(pl.multiple_of(base + t * STEP, STEP), STEP)
                mid[window, :] = got1[window, :] + first_sign[half] * mid[window, :]

            for j, (start, length) in enumerate(pieces2[half]):
                if base < start + length <= base + size:
                    second(half, j).start()

    @pl.when(is_source)
    def _():
        @pl.loop(0, rows - 1)
        def _(k):
            scales(k).wait_send()

    @pl.when(jnp.logical_not(is_source))
    def _():
        scales(0).wait_recv()

    global_col = jnp.where(left, c * local_cols, N // 2 + c * local_cols - W)

    for i in range(len(SECOND)):
        for half in range(2):
            base, size = pieces2[half][i]
            second(half, i).wait_recv()

            @pl.loop(0, size // STEP)
            def _(t):
                here = base + t * STEP
                window = pl.ds(pl.multiple_of(here, STEP), STEP)
                for b in range(local_cols // LANES):
                    lanes = slice(b * LANES, (b + 1) * LANES)
                    value = got2[window, lanes] + second_sign[half] * mid[window, lanes]
                    value = value * (srow[window, :] * cscale[b : b + 1, :])
                    row_index = r * local_rows + here + lax.broadcasted_iota(jnp.int32, value.shape, 0)
                    col_index = global_col + b * LANES + lax.broadcasted_iota(jnp.int32, value.shape, 1)
                    out_ref[window, lanes] = jnp.where(row_index >= col_index, value, jnp.float32(0.0))

    def drained(source, base, size, sem):
        window = pl.ds(base, size)
        pltpu.make_async_remote_copy(
            source.at[window], got1.at[window], sem, recv1.at[0, 0],
            device_id=z_peer, device_id_type=MESH).wait_send()

    for half in range(2):
        drained(x_ref, half * half_rows + FIRST[0], half_rows - FIRST[0], send1.at[half, 1])
        drained(mid, half * half_rows, half_rows, send2.at[half])


def per_device(rows, cols, slab_pair, butterfly_scale):
    local_rows, local_cols = slab_pair.shape
    hbm = pl.BlockSpec(memory_space=pltpu.HBM)
    vmem = pl.BlockSpec(memory_space=pltpu.VMEM)
    s64 = butterfly_scale.reshape(local_rows // LANES, LANES)
    s2 = butterfly_scale.reshape(local_rows // local_cols, local_cols // LANES, LANES)
    block = pltpu.VMEM((local_rows, local_cols), jnp.float32)
    dma = pltpu.SemaphoreType.DMA
    return pl.pallas_call(
        functools.partial(exchange_kernel, rows, cols),
        out_shape=jax.ShapeDtypeStruct(slab_pair.shape, slab_pair.dtype),
        in_specs=[hbm, hbm, hbm],
        out_specs=vmem,
        scratch_shapes=[
            block, block, block,
            pltpu.VMEM((local_rows, LANES), jnp.float32),
            pltpu.VMEM((local_rows // LANES, LANES), jnp.float32),
            pltpu.VMEM((local_cols // LANES, LANES), jnp.float32),
            dma((2, len(FIRST))), dma((2, 2)), dma((2, len(FIRST))), dma((2,)), dma((2, len(SECOND))),
            dma((rows - 1,)), dma, dma((2,)),
            pltpu.SemaphoreType.REGULAR, pltpu.SemaphoreType.REGULAR, pltpu.SemaphoreType.REGULAR,
        ],
        compiler_params=pltpu.CompilerParams(
            collective_id=0, has_side_effects=True, vmem_limit_bytes=40 * 1024 * 1024
        ),
    )(slab_pair, *(pltpu.with_memory_space_constraint(s, pltpu.HBM) for s in (s64, s2)))


def solution(mesh):
    return jax.shard_map(
        functools.partial(per_device, mesh.shape["row"], mesh.shape["col"]),
        mesh=mesh,
        in_specs=(P("row", "col"), P("row")),
        out_specs=P("row", "col"),
        check_vma=False,
    )
```

```python
import functools

import jax
import jax.numpy as jnp
from jax import lax
from jax.experimental import pallas as pl
from jax.experimental.pallas import tpu as pltpu
from jax.sharding import PartitionSpec as P

MESH = pl.DeviceIdType.MESH
N = 65536
W = 2048
FIRST = (128, 1920, 2048)
SECOND = (2048, 1792, 256)
STEP = 128
LANES = 128


def spans(sizes, base):
    out = []
    for size in sizes:
        out.append((base, size))
        base += size
    return out


def exchange_kernel(rows, cols, x_ref, s64_ref, s2_ref, out_ref,
                    mid, got1, got2, srow, s64, cscale,
                    load_sem, send1, recv1, send2, recv2, cs_send, cs_recv,
                    scale_sem, ready_z, ready_x, all_in):
    r = lax.axis_index("row")
    c = lax.axis_index("col")
    local_rows, local_cols = x_ref.shape
    half_rows = local_rows // 2
    pieces1 = spans(FIRST, 0), spans(FIRST, half_rows)
    pieces2 = spans(SECOND, 0), spans(SECOND, half_rows)
    top = r < rows // 2
    left = c < cols // 2
    z_peer = (lax.rem(r + rows // 2, rows), c)
    x_peer = (r, lax.rem(c + cols // 2, cols))
    half_cols = cols // 2
    source_row = jnp.where(left, 0, rows // 2)
    is_source = r == source_row
    hub = is_source & left

    def load(half, i):
        window = pl.ds(*pieces1[half][i])
        return pltpu.make_async_copy(x_ref.at[window], mid.at[window], load_sem.at[half, min(i, 1)])

    def first(half, i):
        window = pl.ds(*pieces1[half][i])
        return pltpu.make_async_remote_copy(
            (x_ref if i else mid).at[window], got1.at[window],
            send1.at[half, min(i, 1)], recv1.at[half, i],
            device_id=(z_peer, x_peer)[half], device_id_type=MESH)

    def second(half, i):
        window = pl.ds(*pieces2[half][i])
        return pltpu.make_async_remote_copy(
            mid.at[window], got2.at[window], send2.at[half], recv2.at[half, i],
            device_id=(x_peer, z_peer)[half], device_id_type=MESH)

    def scales(k):
        return pltpu.make_async_remote_copy(
            cscale, cscale, cs_send, cs_recv,
            device_id=(lax.rem(source_row + 1 + k, rows), c), device_id_type=MESH)

    barrier = pltpu.get_barrier_semaphore()

    def greet(peer):
        pl.semaphore_signal(barrier, inc=1, device_id=peer, device_id_type=MESH)

    def answer(ready, peer):
        pl.semaphore_signal(ready, inc=1, device_id=peer, device_id_type=MESH)

    def send_z():
        load(0, 0).wait()
        for i in range(len(FIRST)):
            first(0, i).start()

    def send_x():
        load(1, 0).wait()
        for i in range(len(FIRST)):
            first(1, i).start()

    load(0, 0).start()
    load(1, 0).start()

    @pl.when(top)
    def _():
        greet(z_peer)

    @pl.when(left)
    def _():
        greet(x_peer)

    @pl.when(jnp.logical_not(hub))
    def _():
        greet((0, lax.rem(c, half_cols)))

    greetings = jnp.where(top, 0, 1) + jnp.where(left, 0, 1)

    @pl.when(greetings > 0)
    def _():
        pl.semaphore_wait(barrier, greetings)

    @pl.when(jnp.logical_not(top))
    def _():
        answer(ready_z, z_peer)

    @pl.when(jnp.logical_not(left))
    def _():
        answer(ready_x, x_peer)
        send_x()

    @pl.when(jnp.logical_not(top))
    def _():
        send_z()

    @pl.when(top)
    def _():
        pl.semaphore_wait(ready_z, 1)
        send_z()

    @pl.when(left)
    def _():
        pl.semaphore_wait(ready_x, 1)
        send_x()

    load_scale = pltpu.make_async_copy(s64_ref, s64, scale_sem)
    load_scale.start()

    for i in range(1, len(FIRST)):
        load(0, i).start()
        load(1, i).start()

    load_scale.wait()

    @pl.loop(0, local_rows // LANES)
    def _(g):
        line = jnp.broadcast_to(s64[pl.ds(g, 1), :], (LANES, LANES))
        srow[pl.ds(pl.multiple_of(g * LANES, LANES), LANES), :] = line.T * jnp.float32(0.5)

    @pl.when(hub)
    def _():
        pl.semaphore_wait(barrier, 2 * rows - 1)
        answer(all_in, (rows // 2, c + half_cols))

    @pl.when(is_source)
    def _():
        own_scale = pltpu.make_async_copy(s2_ref.at[lax.rem(c, half_cols)], cscale, scale_sem)
        own_scale.start()
        own_scale.wait()

        @pl.when(jnp.logical_not(left))
        def _():
            pl.semaphore_wait(all_in, 1)

        @pl.loop(0, rows - 1)
        def _(k):
            scales(k).start()

    z_sign = jnp.where(top, 1.0, -1.0).astype(jnp.float32)
    x_sign = jnp.where(left, 1.0, -1.0).astype(jnp.float32)

    first_sign = z_sign, x_sign
    second_sign = x_sign, z_sign

    for i in range(len(FIRST)):
        for half in range(2):
            base, size = pieces1[half][i]
            first(half, i).wait_recv()
            if i == 1:
                rest = pl.ds(half * half_rows + FIRST[0], half_rows - FIRST[0])
                pltpu.make_async_copy(x_ref.at[rest], mid.at[rest], load_sem.at[half, 1]).wait()
            elif i == 0:
                first(half, i).wait_send()

            @pl.loop(0, size // STEP)
            def _(t):
                window = pl.ds(pl.multiple_of(base + t * STEP, STEP), STEP)
                mid[window, :] = got1[window, :] + first_sign[half] * mid[window, :]

            for j, (start, length) in enumerate(pieces2[half]):
                if base < start + length <= base + size:
                    second(half, j).start()

    @pl.when(is_source)
    def _():
        sent = srow.at[pl.ds(0, (rows - 1) * (local_cols // LANES))]
        pltpu.make_async_remote_copy(
            sent, sent, cs_send, cs_recv, device_id=z_peer, device_id_type=MESH).wait_send()

    @pl.when(jnp.logical_not(is_source))
    def _():
        scales(0).wait_recv()

    global_col = jnp.where(left, c * local_cols, N // 2 + c * local_cols - W)

    for i in range(len(SECOND)):
        for half in range(2):
            base, size = pieces2[half][i]
            second(half, i).wait_recv()

            @pl.loop(0, size // STEP)
            def _(t):
                here = base + t * STEP
                window = pl.ds(pl.multiple_of(here, STEP), STEP)
                for b in range(local_cols // LANES):
                    lanes = slice(b * LANES, (b + 1) * LANES)
                    value = got2[window, lanes] + second_sign[half] * mid[window, lanes]
                    value = value * (srow[window, :] * cscale[b : b + 1, :])
                    row_index = r * local_rows + here + lax.broadcasted_iota(jnp.int32, value.shape, 0)
                    col_index = global_col + b * LANES + lax.broadcasted_iota(jnp.int32, value.shape, 1)
                    out_ref[window, lanes] = jnp.where(row_index >= col_index, value, jnp.float32(0.0))

    def drained(source, base, size, sem):
        window = pl.ds(base, size)
        pltpu.make_async_remote_copy(
            source.at[window], got1.at[window], sem, recv1.at[0, 0],
            device_id=z_peer, device_id_type=MESH).wait_send()

    for half in range(2):
        drained(x_ref, half * half_rows + FIRST[0], half_rows - FIRST[0], send1.at[half, 1])
        drained(mid, half * half_rows, half_rows, send2.at[half])


def per_device(rows, cols, slab_pair, butterfly_scale):
    local_rows, local_cols = slab_pair.shape
    hbm = pl.BlockSpec(memory_space=pltpu.HBM)
    vmem = pl.BlockSpec(memory_space=pltpu.VMEM)
    s64 = butterfly_scale.reshape(local_rows // LANES, LANES)
    s2 = butterfly_scale.reshape(local_rows // local_cols, local_cols // LANES, LANES)
    block = pltpu.VMEM((local_rows, local_cols), jnp.float32)
    dma = pltpu.SemaphoreType.DMA
    return pl.pallas_call(
        functools.partial(exchange_kernel, rows, cols),
        out_shape=jax.ShapeDtypeStruct(slab_pair.shape, slab_pair.dtype),
        in_specs=[hbm, hbm, hbm],
        out_specs=vmem,
        scratch_shapes=[
            block, block, block,
            pltpu.VMEM((local_rows, LANES), jnp.float32),
            pltpu.VMEM((local_rows // LANES, LANES), jnp.float32),
            pltpu.VMEM((local_cols // LANES, LANES), jnp.float32),
            dma((2, 2)), dma((2, 2)), dma((2, len(FIRST))), dma((2,)), dma((2, len(SECOND))),
            dma, dma, dma,
            pltpu.SemaphoreType.REGULAR, pltpu.SemaphoreType.REGULAR, pltpu.SemaphoreType.REGULAR,
        ],
        compiler_params=pltpu.CompilerParams(
            collective_id=0, has_side_effects=True, vmem_limit_bytes=40 * 1024 * 1024
        ),
    )(slab_pair, *(pltpu.with_memory_space_constraint(s, pltpu.HBM) for s in (s64, s2)))


def solution(mesh):
    return jax.shard_map(
        functools.partial(per_device, mesh.shape["row"], mesh.shape["col"]),
        mesh=mesh,
        in_specs=(P("row", "col"), P("row")),
        out_specs=P("row", "col"),
        check_vma=False,
    )
```

```python
import functools

import jax
import jax.numpy as jnp
from jax import lax
from jax.experimental import pallas as pl
from jax.experimental.pallas import tpu as pltpu
from jax.sharding import PartitionSpec as P

MESH = pl.DeviceIdType.MESH
N = 65536
W = 2048
FIRST = (128, 1920, 2048)
SECOND = (2048, 1792, 256)
STEP = 128
LANES = 128
PARTS = 16


def spans(sizes, base):
    out = []
    for size in sizes:
        out.append((base, size))
        base += size
    return out


def exchange_kernel(rows, cols, x_ref, s64_ref, s2_ref, out_ref,
                    mid, got1, got2, srow, s64, cscale,
                    load_sem, send1, recv1, send2, recv2, cs_send, cs_recv,
                    scale_sem, ready_z, ready_x, all_in):
    r = lax.axis_index("row")
    c = lax.axis_index("col")
    local_rows, local_cols = x_ref.shape
    half_rows = local_rows // 2
    pieces1 = spans(FIRST, 0), spans(FIRST, half_rows)
    pieces2 = spans(SECOND, 0), spans(SECOND, half_rows)
    top = r < rows // 2
    left = c < cols // 2
    z_peer = (lax.rem(r + rows // 2, rows), c)
    x_peer = (r, lax.rem(c + cols // 2, cols))
    half_cols = cols // 2
    source_row = jnp.where(left, 0, rows // 2)
    is_source = r == source_row
    hub = is_source & left

    def load(half, i):
        window = pl.ds(*pieces1[half][i])
        return pltpu.make_async_copy(x_ref.at[window], mid.at[window], load_sem.at[half, min(i, 1)])

    def first(half, i):
        window = pl.ds(*pieces1[half][i])
        return pltpu.make_async_remote_copy(
            (x_ref if i else mid).at[window], got1.at[window],
            send1.at[half, min(i, 1)], recv1.at[half, i],
            device_id=(z_peer, x_peer)[half], device_id_type=MESH)

    def second(half, i):
        window = pl.ds(*pieces2[half][i])
        return pltpu.make_async_remote_copy(
            mid.at[window], got2.at[window], send2.at[half], recv2.at[half, i],
            device_id=(x_peer, z_peer)[half], device_id_type=MESH)

    def scales(k):
        return pltpu.make_async_remote_copy(
            cscale, cscale, cs_send, cs_recv,
            device_id=(lax.rem(source_row + 1 + k, rows), c), device_id_type=MESH)

    barrier = pltpu.get_barrier_semaphore()

    def greet(peer):
        pl.semaphore_signal(barrier, inc=1, device_id=peer, device_id_type=MESH)

    def answer(ready, peer):
        pl.semaphore_signal(ready, inc=1, device_id=peer, device_id_type=MESH)

    def send_z():
        load(0, 0).wait()
        for i in range(len(FIRST)):
            first(0, i).start()

    def send_x():
        load(1, 0).wait()
        for i in range(len(FIRST)):
            first(1, i).start()

    load(0, 0).start()
    load(1, 0).start()

    @pl.when(top)
    def _():
        greet(z_peer)

    @pl.when(left)
    def _():
        greet(x_peer)

    @pl.when(jnp.logical_not(hub))
    def _():
        greet((0, lax.rem(c, half_cols)))

    greetings = jnp.where(top, 0, 1) + jnp.where(left, 0, 1)

    @pl.when(greetings > 0)
    def _():
        pl.semaphore_wait(barrier, greetings)

    @pl.when(jnp.logical_not(top))
    def _():
        answer(ready_z, z_peer)

    @pl.when(jnp.logical_not(left))
    def _():
        answer(ready_x, x_peer)
        send_x()

    @pl.when(jnp.logical_not(top))
    def _():
        send_z()

    @pl.when(top)
    def _():
        pl.semaphore_wait(ready_z, 1)
        send_z()

    @pl.when(left)
    def _():
        pl.semaphore_wait(ready_x, 1)
        send_x()

    load_scale = pltpu.make_async_copy(s64_ref, s64, scale_sem)
    load_scale.start()

    for i in range(1, len(FIRST)):
        load(0, i).start()
        load(1, i).start()

    load_scale.wait()

    @pl.loop(0, local_rows // LANES)
    def _(g):
        line = jnp.broadcast_to(s64[pl.ds(g, 1), :], (LANES, LANES))
        srow[pl.ds(pl.multiple_of(g * LANES, LANES), LANES), :] = line.T * jnp.float32(0.5)

    @pl.when(hub)
    def _():
        pl.semaphore_wait(barrier, 2 * rows - 1)
        answer(all_in, (rows // 2, c + half_cols))

    @pl.when(is_source)
    def _():
        own_scale = pltpu.make_async_copy(s2_ref.at[lax.rem(c, half_cols)], cscale, scale_sem)
        own_scale.start()
        own_scale.wait()

        @pl.when(jnp.logical_not(left))
        def _():
            pl.semaphore_wait(all_in, 1)

        @pl.loop(0, rows - 1)
        def _(k):
            scales(k).start()

    z_sign = jnp.where(top, 1.0, -1.0).astype(jnp.float32)
    x_sign = jnp.where(left, 1.0, -1.0).astype(jnp.float32)

    first_sign = z_sign, x_sign
    second_sign = x_sign, z_sign

    for i in range(len(FIRST)):
        for half in range(2):
            base, size = pieces1[half][i]
            first(half, i).wait_recv()
            if i == 1:
                rest = pl.ds(half * half_rows + FIRST[0], half_rows - FIRST[0])
                pltpu.make_async_copy(x_ref.at[rest], mid.at[rest], load_sem.at[half, 1]).wait()
            elif i == 0:
                first(half, i).wait_send()

            @pl.loop(0, size // STEP)
            def _(t):
                window = pl.ds(pl.multiple_of(base + t * STEP, STEP), STEP)
                mid[window, :] = got1[window, :] + first_sign[half] * mid[window, :]

            for j, (start, length) in enumerate(pieces2[half]):
                if base < start + length <= base + size:
                    second(half, j).start()

    @pl.when(is_source)
    def _():
        sent = srow.at[pl.ds(0, (rows - 1) * (local_cols // LANES))]
        pltpu.make_async_remote_copy(
            sent, sent, cs_send, cs_recv, device_id=z_peer, device_id_type=MESH).wait_send()

    @pl.when(jnp.logical_not(is_source))
    def _():
        scales(0).wait_recv()

    global_col = jnp.where(left, c * local_cols, N // 2 + c * local_cols - W)

    for i in range(len(SECOND)):
        for half in range(2):
            base, size = pieces2[half][i]
            second(half, i).wait_recv()

            @pl.loop(0, size // STEP)
            def _(t):
                here = base + t * STEP
                window = pl.ds(pl.multiple_of(here, STEP), STEP)
                for b in range(local_cols // LANES):
                    lanes = slice(b * LANES, (b + 1) * LANES)
                    value = got2[window, lanes] + second_sign[half] * mid[window, lanes]
                    value = value * (srow[window, :] * cscale[b : b + 1, :])
                    row_index = r * local_rows + here + lax.broadcasted_iota(jnp.int32, value.shape, 0)
                    col_index = global_col + b * LANES + lax.broadcasted_iota(jnp.int32, value.shape, 1)
                    out_ref[window, lanes] = jnp.where(row_index >= col_index, value, jnp.float32(0.0))

    def drained(source, base, size, sem):
        window = pl.ds(base, size)
        pltpu.make_async_remote_copy(
            source.at[window], got1.at[window], sem, recv1.at[0, 0],
            device_id=z_peer, device_id_type=MESH).wait_send()

    for half in range(2):
        drained(x_ref, half * half_rows + FIRST[0], half_rows - FIRST[0], send1.at[half, 1])
        drained(mid, half * half_rows, half_rows, send2.at[half])


def per_device(rows, cols, slab_pair, butterfly_scale):
    local_rows, local_cols = slab_pair.shape
    hbm = pl.BlockSpec(memory_space=pltpu.HBM)
    vmem = pl.BlockSpec(memory_space=pltpu.VMEM)
    s64 = butterfly_scale.reshape(local_rows // LANES, LANES)
    s2 = butterfly_scale.reshape(local_rows // local_cols, local_cols // LANES, LANES)
    block = pltpu.VMEM((local_rows, local_cols), jnp.float32)
    dma = pltpu.SemaphoreType.DMA
    mixed = pl.pallas_call(
        functools.partial(exchange_kernel, rows, cols),
        out_shape=jax.ShapeDtypeStruct(slab_pair.shape, slab_pair.dtype),
        in_specs=[hbm, hbm, hbm],
        out_specs=vmem,
        scratch_shapes=[
            block, block, block,
            pltpu.VMEM((local_rows, LANES), jnp.float32),
            pltpu.VMEM((local_rows // LANES, LANES), jnp.float32),
            pltpu.VMEM((local_cols // LANES, LANES), jnp.float32),
            dma((2, 2)), dma((2, 2)), dma((2, len(FIRST))), dma((2,)), dma((2, len(SECOND))),
            dma, dma, dma,
            pltpu.SemaphoreType.REGULAR, pltpu.SemaphoreType.REGULAR, pltpu.SemaphoreType.REGULAR,
        ],
        compiler_params=pltpu.CompilerParams(
            collective_id=0, has_side_effects=True, vmem_limit_bytes=40 * 1024 * 1024
        ),
    )(slab_pair, *(pltpu.with_memory_space_constraint(s, pltpu.HBM) for s in (s64, s2)))

    def write_out(from_ref, to_ref, sem):
        for k in range(PARTS):
            window = pl.ds(k * (local_rows // PARTS), local_rows // PARTS)
            pltpu.make_async_copy(from_ref.at[window], to_ref.at[window], sem).start()
        pltpu.make_async_copy(from_ref, to_ref, sem).wait()

    return pl.pallas_call(
        write_out,
        out_shape=jax.ShapeDtypeStruct(slab_pair.shape, slab_pair.dtype),
        in_specs=[vmem],
        out_specs=hbm,
        scratch_shapes=[dma],
        compiler_params=pltpu.CompilerParams(vmem_limit_bytes=1024 * 1024),
    )(mixed)


def solution(mesh):
    return jax.shard_map(
        functools.partial(per_device, mesh.shape["row"], mesh.shape["col"]),
        mesh=mesh,
        in_specs=(P("row", "col"), P("row")),
        out_specs=P("row", "col"),
        check_vma=False,
    )
```

```python
import functools

import jax
import jax.numpy as jnp
from jax import lax
from jax.experimental import pallas as pl
from jax.experimental.pallas import tpu as pltpu
from jax.sharding import PartitionSpec as P

MESH = pl.DeviceIdType.MESH
N = 65536
W = 2048
FIRST = (128, 1920, 2048)
SECOND = (2048, 1792, 256)
STEP = 128
LANES = 128
PARTS = 32


def spans(sizes, base):
    out = []
    for size in sizes:
        out.append((base, size))
        base += size
    return out


def exchange_kernel(rows, cols, x_ref, s64_ref, s2_ref, out_ref,
                    mid, got1, got2, srow, s64, cscale,
                    load_sem, send1, recv1, send2, recv2, cs_send, cs_recv,
                    scale_sem, ready_z, ready_x, all_in):
    r = lax.axis_index("row")
    c = lax.axis_index("col")
    local_rows, local_cols = x_ref.shape
    half_rows = local_rows // 2
    pieces1 = spans(FIRST, 0), spans(FIRST, half_rows)
    pieces2 = spans(SECOND, 0), spans(SECOND, half_rows)
    top = r < rows // 2
    left = c < cols // 2
    z_peer = (lax.rem(r + rows // 2, rows), c)
    x_peer = (r, lax.rem(c + cols // 2, cols))
    half_cols = cols // 2
    source_row = jnp.where(left, 0, rows // 2)
    is_source = r == source_row
    hub = is_source & left

    def load(half, i):
        window = pl.ds(*pieces1[half][i])
        return pltpu.make_async_copy(x_ref.at[window], mid.at[window], load_sem.at[half, min(i, 1)])

    def first(half, i):
        window = pl.ds(*pieces1[half][i])
        return pltpu.make_async_remote_copy(
            (x_ref if i else mid).at[window], got1.at[window],
            send1.at[half, min(i, 1)], recv1.at[half, i],
            device_id=(z_peer, x_peer)[half], device_id_type=MESH)

    def second(half, i):
        window = pl.ds(*pieces2[half][i])
        return pltpu.make_async_remote_copy(
            mid.at[window], got2.at[window], send2.at[half], recv2.at[half, i],
            device_id=(x_peer, z_peer)[half], device_id_type=MESH)

    def scales(k):
        return pltpu.make_async_remote_copy(
            cscale, cscale, cs_send, cs_recv,
            device_id=(lax.rem(source_row + 1 + k, rows), c), device_id_type=MESH)

    barrier = pltpu.get_barrier_semaphore()

    def greet(peer):
        pl.semaphore_signal(barrier, inc=1, device_id=peer, device_id_type=MESH)

    def answer(ready, peer):
        pl.semaphore_signal(ready, inc=1, device_id=peer, device_id_type=MESH)

    def send_z():
        load(0, 0).wait()
        for i in range(len(FIRST)):
            first(0, i).start()

    def send_x():
        load(1, 0).wait()
        for i in range(len(FIRST)):
            first(1, i).start()

    load(0, 0).start()
    load(1, 0).start()

    @pl.when(top)
    def _():
        greet(z_peer)

    @pl.when(left)
    def _():
        greet(x_peer)

    @pl.when(jnp.logical_not(hub))
    def _():
        greet((0, lax.rem(c, half_cols)))

    greetings = jnp.where(top, 0, 1) + jnp.where(left, 0, 1)

    @pl.when(greetings > 0)
    def _():
        pl.semaphore_wait(barrier, greetings)

    @pl.when(jnp.logical_not(top))
    def _():
        answer(ready_z, z_peer)

    @pl.when(jnp.logical_not(left))
    def _():
        answer(ready_x, x_peer)
        send_x()

    @pl.when(jnp.logical_not(top))
    def _():
        send_z()

    @pl.when(top)
    def _():
        pl.semaphore_wait(ready_z, 1)
        send_z()

    @pl.when(left)
    def _():
        pl.semaphore_wait(ready_x, 1)
        send_x()

    load_scale = pltpu.make_async_copy(s64_ref, s64, scale_sem)
    load_scale.start()

    for i in range(1, len(FIRST)):
        load(0, i).start()
        load(1, i).start()

    load_scale.wait()

    @pl.loop(0, local_rows // LANES)
    def _(g):
        line = jnp.broadcast_to(s64[pl.ds(g, 1), :], (LANES, LANES))
        srow[pl.ds(pl.multiple_of(g * LANES, LANES), LANES), :] = line.T * jnp.float32(0.5)

    @pl.when(hub)
    def _():
        pl.semaphore_wait(barrier, 2 * rows - 1)
        answer(all_in, (rows // 2, c + half_cols))

    @pl.when(is_source)
    def _():
        own_scale = pltpu.make_async_copy(s2_ref.at[lax.rem(c, half_cols)], cscale, scale_sem)
        own_scale.start()
        own_scale.wait()

        @pl.when(jnp.logical_not(left))
        def _():
            pl.semaphore_wait(all_in, 1)

        @pl.loop(0, rows - 1)
        def _(k):
            scales(k).start()

    z_sign = jnp.where(top, 1.0, -1.0).astype(jnp.float32)
    x_sign = jnp.where(left, 1.0, -1.0).astype(jnp.float32)

    first_sign = z_sign, x_sign
    second_sign = x_sign, z_sign

    for i in range(len(FIRST)):
        for half in range(2):
            base, size = pieces1[half][i]
            first(half, i).wait_recv()
            if i == 1:
                rest = pl.ds(half * half_rows + FIRST[0], half_rows - FIRST[0])
                pltpu.make_async_copy(x_ref.at[rest], mid.at[rest], load_sem.at[half, 1]).wait()
            elif i == 0:
                first(half, i).wait_send()

            @pl.loop(0, size // STEP)
            def _(t):
                window = pl.ds(pl.multiple_of(base + t * STEP, STEP), STEP)
                mid[window, :] = got1[window, :] + first_sign[half] * mid[window, :]

            for j, (start, length) in enumerate(pieces2[half]):
                if base < start + length <= base + size:
                    second(half, j).start()

    @pl.when(is_source)
    def _():
        sent = srow.at[pl.ds(0, (rows - 1) * (local_cols // LANES))]
        pltpu.make_async_remote_copy(
            sent, sent, cs_send, cs_recv, device_id=z_peer, device_id_type=MESH).wait_send()

    @pl.when(jnp.logical_not(is_source))
    def _():
        scales(0).wait_recv()

    global_col = jnp.where(left, c * local_cols, N // 2 + c * local_cols - W)

    for i in range(len(SECOND)):
        for half in range(2):
            base, size = pieces2[half][i]
            second(half, i).wait_recv()

            @pl.loop(0, size // STEP)
            def _(t):
                here = base + t * STEP
                window = pl.ds(pl.multiple_of(here, STEP), STEP)
                for b in range(local_cols // LANES):
                    lanes = slice(b * LANES, (b + 1) * LANES)
                    value = got2[window, lanes] + second_sign[half] * mid[window, lanes]
                    value = value * (srow[window, :] * cscale[b : b + 1, :])
                    row_index = r * local_rows + here + lax.broadcasted_iota(jnp.int32, value.shape, 0)
                    col_index = global_col + b * LANES + lax.broadcasted_iota(jnp.int32, value.shape, 1)
                    out_ref[window, lanes] = jnp.where(row_index >= col_index, value, jnp.float32(0.0))

    def drained(source, base, size, sem):
        window = pl.ds(base, size)
        pltpu.make_async_remote_copy(
            source.at[window], got1.at[window], sem, recv1.at[0, 0],
            device_id=z_peer, device_id_type=MESH).wait_send()

    for half in range(2):
        drained(x_ref, half * half_rows + FIRST[0], half_rows - FIRST[0], send1.at[half, 1])
        drained(mid, half * half_rows, half_rows, send2.at[half])


def per_device(rows, cols, slab_pair, butterfly_scale):
    local_rows, local_cols = slab_pair.shape
    hbm = pl.BlockSpec(memory_space=pltpu.HBM)
    vmem = pl.BlockSpec(memory_space=pltpu.VMEM)
    s64 = butterfly_scale.reshape(local_rows // LANES, LANES)
    s2 = butterfly_scale.reshape(local_rows // local_cols, local_cols // LANES, LANES)
    block = pltpu.VMEM((local_rows, local_cols), jnp.float32)
    dma = pltpu.SemaphoreType.DMA
    mixed = pl.pallas_call(
        functools.partial(exchange_kernel, rows, cols),
        out_shape=jax.ShapeDtypeStruct(slab_pair.shape, slab_pair.dtype),
        in_specs=[hbm, hbm, hbm],
        out_specs=vmem,
        scratch_shapes=[
            block, block, block,
            pltpu.VMEM((local_rows, LANES), jnp.float32),
            pltpu.VMEM((local_rows // LANES, LANES), jnp.float32),
            pltpu.VMEM((local_cols // LANES, LANES), jnp.float32),
            dma((2, 2)), dma((2, 2)), dma((2, len(FIRST))), dma((2,)), dma((2, len(SECOND))),
            dma, dma, dma,
            pltpu.SemaphoreType.REGULAR, pltpu.SemaphoreType.REGULAR, pltpu.SemaphoreType.REGULAR,
        ],
        compiler_params=pltpu.CompilerParams(
            collective_id=0, has_side_effects=True, vmem_limit_bytes=40 * 1024 * 1024
        ),
    )(slab_pair, *(pltpu.with_memory_space_constraint(s, pltpu.HBM) for s in (s64, s2)))

    def write_out(from_ref, to_ref, sem):
        for k in range(PARTS):
            window = pl.ds(k * (local_rows // PARTS), local_rows // PARTS)
            pltpu.make_async_copy(from_ref.at[window], to_ref.at[window], sem).start()
        pltpu.make_async_copy(from_ref, to_ref, sem).wait()

    return pl.pallas_call(
        write_out,
        out_shape=jax.ShapeDtypeStruct(slab_pair.shape, slab_pair.dtype),
        in_specs=[vmem],
        out_specs=hbm,
        scratch_shapes=[dma],
        compiler_params=pltpu.CompilerParams(vmem_limit_bytes=1024 * 1024),
    )(mixed)


def solution(mesh):
    return jax.shard_map(
        functools.partial(per_device, mesh.shape["row"], mesh.shape["col"]),
        mesh=mesh,
        in_specs=(P("row", "col"), P("row")),
        out_specs=P("row", "col"),
        check_vma=False,
    )
```
